32 devices in a mesh: dp: 8 (over y, x, core), head: 4 (over z).
Axes of the slice: x: 2, y: 2, z: 4, core: 2. Of those that a mesh axis runs over, the one named last changes fastest.
Arguments:
- layer_input_rows: bfloat16 [16384, 1024], P(('dp', 'head')), may hold values from -6 to 6
- cotangent: bfloat16 [16384, 1024], P(('dp', 'head')), may hold values from -6 to 6
- lengths: int32 [16], P('dp'), may hold values from 128 to 1024, as said below
- layernorm_gain: float32 [2, 1024], P(None, ('dp', 'head')), may hold values from 0.5 to 1.5
- layernorm_bias: float32 [2, 1024], P(None, ('dp', 'head')), may hold values from -1.5 to 1.5
- frozen_projection_weight: float32 [1024, 3, 1024], P('dp', None, 'head'), may hold values from -0.1875 to 0.1875
- projection_bias: float32 [3, 16, 64], P(None, 'head', 'dp'), may hold values from -1.5 to 1.5
- adapter_project_first: float32 [3, 1024, 128], P(None, ('dp', 'head')), may hold values from -0.1875 to 0.1875
- adapter_project_second: float32 [3, 128, 1024], P(None, 'dp', 'head'), may hold values from -0.5 to 0.5
- frozen_output_weight: float32 [1024, 1024], P('head', 'dp'), may hold values from -0.75 to 0.75
- adapter_output_first: float32 [1024, 128], P('head', 'dp'), may hold values from -0.75 to 0.75
- adapter_output_second: float32 [128, 1024], P(None, ('dp', 'head')), may hold values from -0.5 to 0.5
- frozen_up_weight: float32 [1024, 4096], P('dp', 'head'), may hold values from -0.1875 to 0.1875
- hidden_bias: float32 [64, 64], P('head', 'dp'), may hold values from -1.5 to 1.5
- adapter_up_first: float32 [1024, 128], P(('dp', 'head')), may hold values from -0.1875 to 0.1875
- adapter_up_second: float32 [128, 4096], P('dp', 'head'), may hold values from -0.5 to 0.5
- frozen_down_weight: float32 [4096, 1024], P('head', 'dp'), may hold values from -0.09375 to 0.09375
- adapter_down_first: float32 [4096, 128], P('head', 'dp'), may hold values from -0.09375 to 0.09375
- adapter_down_second: float32 [128, 1024], P(None, ('dp', 'head')), may hold values from -0.5 to 0.5
- branch_output_bias: float32 [2, 1024], P(None, ('dp', 'head')), may hold values from -1.5 to 1.5
Outputs:
- layer_output: bfloat16 [16384, 1024], P(('dp', 'head'))
- grad_input: float32 [16384, 1024], P(('dp', 'head'))
- gradient_layernorm_gain: float32 [2, 1024], P(None, ('dp', 'head'))
- gradient_layernorm_bias: float32 [2, 1024], P(None, ('dp', 'head'))
- gradient_projection_bias: float32 [3, 16, 64], P(None, 'head', 'dp')
- gradient_adapter_project_first: float32 [3, 1024, 128], P(None, ('dp', 'head'))
- gradient_adapter_project_second: float32 [3, 128, 1024], P(None, 'dp', 'head')
- gradient_adapter_output_first: float32 [1024, 128], P('head', 'dp')
- gradient_adapter_output_second: float32 [128, 1024], P(None, ('dp', 'head'))
- gradient_hidden_bias: float32 [64, 64], P('head', 'dp')
- gradient_adapter_up_first: float32 [1024, 128], P(('dp', 'head'))
- gradient_adapter_up_second: float32 [128, 4096], P('dp', 'head')
- gradient_adapter_down_first: float32 [4096, 128], P('head', 'dp')
- gradient_adapter_down_second: float32 [128, 1024], P(None, ('dp', 'head'))
- gradient_branch_bias: float32 [2, 1024], P(None, ('dp', 'head'))
The draws below stay inside these ranges and needn't reach their ends.
Inputs may be any that keep to these rules, and one draw needn't show every extreme that they name: lengths[i] counts the real tokens at the start of sequence i; the slots after them are padding; some sequence has exactly 1024.
All inputs are finite; a program needn't handle non-finite values.
Results may differ from the reference program's by a relative error of at most 0.012.
Values may be sent and summed in bfloat16 or wider, within the bound.
A program may use at most 192 MiB of HBM per device.

```python
import math
import jax
import jax.numpy as jnp
from jax import lax

MODEL_WIDTH = 1024
NH = 16
HD = 64
HIDDEN_UNITS = 4096
ADAPTER_RANK = 128
ADAPTER_ALPHA = 32
ROW_LEN = 1024
SEQS = 2
ROWS = 16
TOKEN_SLOTS = 16384
N_DP = 8


def draw_lengths(key, part):
    first_key, second_key, third_key = jax.random.split(jax.random.fold_in(key, 7), 3)
    tiers = jax.random.randint(first_key, (ROWS,), 0, 8)
    lower = jnp.where(tiers < 2, ROW_LEN // 8, jnp.where(tiers < 4, ROW_LEN // 4, jnp.where(tiers < 7, ROW_LEN // 2, ROW_LEN)))
    upper = jnp.where(tiers < 2, ROW_LEN // 4, jnp.where(tiers < 4, ROW_LEN // 2, jnp.where(tiers < 7, ROW_LEN, ROW_LEN + 1)))
    drawn = jax.random.randint(second_key, (ROWS,), lower, upper)
    chosen = jax.random.randint(third_key, (), 0, ROWS)
    return jnp.where(jnp.arange(ROWS) == chosen, ROW_LEN, drawn).astype(jnp.int32)


def strengthened(entries, key, source, target, blocks, factor):
    owner, partner = [(jnp.arange(entries.shape[axis_at]) // (entries.shape[axis_at] // blocks)).reshape([-1 if axis == axis_at else 1 for axis in range(entries.ndim)]) for axis_at in (source, target)]
    chosen = jax.random.permutation(key, blocks)[partner]
    strong = (owner == chosen) | (owner == (partner + blocks // 2) % blocks)
    return jnp.where(strong, factor * entries, entries)


def block_levels(key, shape, cuts, low, top_value):
    gain, own = 1.0, jax.random.fold_in(key, 6)
    for dim, blocks in cuts:
        steps = jnp.exp(jax.random.uniform(jax.random.fold_in(own, dim), (blocks,), jnp.float32, low / len(cuts), top_value / len(cuts)))
        gain = gain * jnp.repeat(steps, shape[dim] // blocks).reshape([-1 if axis == dim else 1 for axis in range(len(shape))])
    return gain


def noise(own_key, extent, scale, bound, shards=(), kind=jnp.bfloat16):
    array = jax.random.normal(own_key, extent, jnp.float32) * scale
    if len(shards) > 0:
        array = block_levels(own_key, extent, shards, -0.22, 0.18) * array
    return jnp.clip(array, min=-bound, max=bound).astype(kind)


def gaussian_with(rng, dims, deviation, limit, cuts, heavy, kind=jnp.bfloat16):
    values = deviation * jax.random.normal(rng, dims, jnp.float32)
    if cuts:
        values = values * block_levels(rng, dims, cuts, -0.22, 0.18)
    return jnp.clip(strengthened(values, jax.random.fold_in(rng, 3), *heavy), -limit, limit).astype(kind)


def setup_inputs(seed: int = 0) -> dict:
    seeds = jax.random.split(jax.random.key(seed), 21)
    layer_input_rows = noise(seeds[0], (TOKEN_SLOTS, MODEL_WIDTH), 1.0, 6.0, ((0, 32),))
    cotangent = gaussian_with(seeds[1], (TOKEN_SLOTS, MODEL_WIDTH), 1.0, 6.0, ((0, 32),), (0, 1, 32, 2.75))
    lengths = draw_lengths(jax.random.fold_in(seeds[20], 71), 0)
    layernorm_gain = jnp.clip(1.0 + 0.1 * jax.random.normal(seeds[3], (2, MODEL_WIDTH), jnp.float32), 0.5, 1.5)
    layernorm_bias = noise(seeds[4], (2, MODEL_WIDTH), 0.3, 1.5, ((1, 32),), jnp.float32)
    frozen_projection_weight = noise(seeds[5], (MODEL_WIDTH, 3, MODEL_WIDTH), MODEL_WIDTH ** -0.5, 0.1875, ((0, 8), (2, 4)), jnp.float32)
    projection_bias = noise(seeds[6], (3, NH, HD), 0.3, 1.5, ((1, 4), (2, 8)), jnp.float32)
    adapter_project_first = noise(seeds[7], (3, MODEL_WIDTH, ADAPTER_RANK), MODEL_WIDTH ** -0.5, 0.1875, ((1, 32),), jnp.float32)
    adapter_project_second = noise(seeds[8], (3, ADAPTER_RANK, MODEL_WIDTH), ADAPTER_RANK ** -0.5, 0.5, ((1, 8), (2, 4)), jnp.float32)
    frozen_output_weight = noise(seeds[9], (MODEL_WIDTH, MODEL_WIDTH), (MODEL_WIDTH // 16) ** -0.5, 0.75, ((0, 4), (1, 8)), jnp.float32)
    adapter_output_first = noise(seeds[10], (MODEL_WIDTH, ADAPTER_RANK), (MODEL_WIDTH // 16) ** -0.5, 0.75, ((0, 4), (1, 8)), jnp.float32)
    adapter_output_second = noise(seeds[11], (ADAPTER_RANK, MODEL_WIDTH), ADAPTER_RANK ** -0.5, 0.5, ((1, 32),), jnp.float32)
    frozen_up_weight = noise(seeds[12], (MODEL_WIDTH, HIDDEN_UNITS), MODEL_WIDTH ** -0.5, 0.1875, ((0, 8), (1, 4)), jnp.float32)
    hidden_bias = noise(seeds[13], (HIDDEN_UNITS // HD, HD), 0.3, 1.5, ((0, 4), (1, 8)), jnp.float32)
    adapter_up_first = noise(seeds[14], (MODEL_WIDTH, ADAPTER_RANK), MODEL_WIDTH ** -0.5, 0.1875, ((0, 32),), jnp.float32)
    adapter_up_second = noise(seeds[15], (ADAPTER_RANK, HIDDEN_UNITS), ADAPTER_RANK ** -0.5, 0.5, ((0, 8), (1, 4)), jnp.float32)
    frozen_down_weight = noise(seeds[16], (HIDDEN_UNITS, MODEL_WIDTH), HIDDEN_UNITS ** -0.5, 0.09375, ((0, 4), (1, 8)), jnp.float32)
    adapter_down_first = noise(seeds[17], (HIDDEN_UNITS, ADAPTER_RANK), HIDDEN_UNITS ** -0.5, 0.09375, ((0, 4), (1, 8)), jnp.float32)
    adapter_down_second = noise(seeds[18], (ADAPTER_RANK, MODEL_WIDTH), ADAPTER_RANK ** -0.5, 0.5, ((1, 32),), jnp.float32)
    branch_output_bias = noise(seeds[19], (2, MODEL_WIDTH), 0.3, 1.5, ((1, 32),), jnp.float32)
    return dict(layer_input_rows=layer_input_rows, cotangent=cotangent, lengths=lengths, layernorm_gain=layernorm_gain, layernorm_bias=layernorm_bias, frozen_projection_weight=frozen_projection_weight, projection_bias=projection_bias, adapter_project_first=adapter_project_first, adapter_project_second=adapter_project_second, frozen_output_weight=frozen_output_weight, adapter_output_first=adapter_output_first, adapter_output_second=adapter_output_second, frozen_up_weight=frozen_up_weight, hidden_bias=hidden_bias, adapter_up_first=adapter_up_first, adapter_up_second=adapter_up_second, frozen_down_weight=frozen_down_weight, adapter_down_first=adapter_down_first, adapter_down_second=adapter_down_second, branch_output_bias=branch_output_bias)


@jax.custom_vjp
def lowrank_path(v):
    return lax.optimization_barrier(v.astype(jnp.bfloat16)).astype(jnp.float32)

@jax.custom_vjp
def lowrank_backward(v):
    return v

def low_keep(v):
    return (lowrank_path(v), None)

def low_pass(kept, grad):
    return (grad,)

def back_keep(v):
    return (v, None)

def back_low(kept, grad):
    return (lowrank_path(grad),)
lowrank_path.defvjp(low_keep, low_pass)
lowrank_backward.defvjp(back_keep, back_low)
FULL_PRECISION = lax.Precision.HIGHEST
NORM_EPSILON = 1e-05
NEG_FILL = -1e+30

def matrix_product(left, right):
    return jnp.dot(left, right, precision=FULL_PRECISION, preferred_element_type=jnp.float32)

def rotary_tables():
    turned = HD // 4
    half_turn = turned // 2
    freqs = 10000.0 ** (-(jnp.arange(half_turn, dtype=jnp.float32) * 2.0 / turned))
    angles = jnp.arange(ROW_LEN, dtype=jnp.float32)[:, None] * freqs[None, :]
    return (jnp.cos(angles)[:, None, :], jnp.sin(angles)[:, None, :])

def turn(values, cosine, sine):
    half_turn = cosine.shape[-1]
    first = values[..., :half_turn]
    second = values[..., half_turn:2 * half_turn]
    rest = values[..., 2 * half_turn:]
    return jnp.concatenate([first * cosine - second * sine, second * cosine + first * sine, rest], axis=-1)

def attend_row(row):
    queries, keys, values, length = row
    positions = jnp.arange(ROW_LEN)
    raw = jnp.einsum('qhd,khd->hqk', queries, keys, precision=FULL_PRECISION) / math.sqrt(HD)
    allowed = positions[None, :] <= positions[:, None]
    scores = jnp.where(allowed[None], lowrank_backward(raw), NEG_FILL)
    weights = jax.nn.softmax(scores, axis=-1)
    attention_context = jnp.einsum('hqk,khd->qhd', lowrank_path(weights), values, precision=FULL_PRECISION)
    valid = (positions < length).astype(attention_context.dtype)
    return attention_context * valid[:, None, None]

def forward(rows, lengths, frozen, training_step):
    frozen_projection_weight, frozen_output_weight, frozen_up_weight, frozen_down_weight = [lowrank_path(current_item) for current_item in frozen]
    layernorm_gain, layernorm_bias, projection_bias, adapter_project_first, adapter_project_second, adapter_output_first, adapter_output_second, hidden_bias, adapter_up_first, adapter_up_second, adapter_down_first, adapter_down_second, branch_output_bias = [lowrank_path(current_item) for current_item in training_step]
    adapter_scale = ADAPTER_ALPHA / ADAPTER_RANK
    centered_rows = rows - lax.optimization_barrier(jnp.mean(rows, axis=-1, keepdims=True))
    standardized_rows = centered_rows * lax.rsqrt(lax.optimization_barrier(jnp.mean(centered_rows * centered_rows, axis=-1, keepdims=True)) + NORM_EPSILON)
    attention_normed = lowrank_path(standardized_rows * layernorm_gain[0] + layernorm_bias[0])
    feedforward_normed = lowrank_path(standardized_rows * layernorm_gain[1] + layernorm_bias[1])
    projection_lowrank = lowrank_backward(lowrank_path(jnp.einsum('po,von->pvn', attention_normed, adapter_project_first, precision=FULL_PRECISION)))
    projected_rows = jnp.einsum('td,dce->tce', attention_normed, frozen_projection_weight, precision=FULL_PRECISION) + projection_bias.reshape(3, MODEL_WIDTH)
    projected_rows = projected_rows + adapter_scale * jnp.einsum('qpf,pfo->qpo', projection_lowrank, adapter_project_second, precision=FULL_PRECISION)
    projected_rows = lowrank_backward(projected_rows).reshape(SEQS, ROW_LEN, 3, NH, HD)
    cosine, sine = rotary_tables()
    queries = lowrank_path(turn(projected_rows[:, :, 0], cosine, sine))
    keys = lowrank_path(turn(projected_rows[:, :, 1], cosine, sine))
    values = lowrank_path(projected_rows[:, :, 2])
    attention_context = lax.map(jax.checkpoint(attend_row), (queries, keys, values, lengths))
    attention_context = lowrank_backward(lowrank_path(attention_context.reshape(SEQS * ROW_LEN, MODEL_WIDTH)))
    attention_lowrank = lowrank_backward(lowrank_path(matrix_product(attention_context, adapter_output_first)))
    attention_branch = matrix_product(attention_context, frozen_output_weight) + adapter_scale * matrix_product(attention_lowrank, adapter_output_second)
    up_lowrank = lowrank_backward(lowrank_path(matrix_product(feedforward_normed, adapter_up_first)))
    preactivation = matrix_product(feedforward_normed, frozen_up_weight) + hidden_bias.reshape(HIDDEN_UNITS) + adapter_scale * matrix_product(up_lowrank, adapter_up_second)
    preactivation = lowrank_backward(preactivation)
    hidden_units_rows = lowrank_path(jax.nn.gelu(preactivation, approximate=False))
    down_lowrank = lowrank_backward(lowrank_path(matrix_product(hidden_units_rows, adapter_down_first)))
    feedforward_branch = matrix_product(hidden_units_rows, frozen_down_weight) + adapter_scale * matrix_product(down_lowrank, adapter_down_second)
    return rows + attention_branch + feedforward_branch + branch_output_bias[0] + branch_output_bias[1]

def reference(layer_input_rows, cotangent, lengths, layernorm_gain, layernorm_bias, frozen_projection_weight, projection_bias, adapter_project_first, adapter_project_second, frozen_output_weight, adapter_output_first, adapter_output_second, frozen_up_weight, hidden_bias, adapter_up_first, adapter_up_second, frozen_down_weight, adapter_down_first, adapter_down_second, branch_output_bias):
    frozen = (frozen_projection_weight, frozen_output_weight, frozen_up_weight, frozen_down_weight)
    training_step = (layernorm_gain, layernorm_bias, projection_bias, adapter_project_first, adapter_project_second, adapter_output_first, adapter_output_second, hidden_bias, adapter_up_first, adapter_up_second, adapter_down_first, adapter_down_second, branch_output_bias)
    rows_all = layer_input_rows.astype(jnp.float32).reshape(N_DP, SEQS * ROW_LEN, MODEL_WIDTH)
    grads_all = cotangent.astype(jnp.float32).reshape(N_DP, SEQS * ROW_LEN, MODEL_WIDTH)
    lengths_all = lengths.reshape(N_DP, SEQS)

    def one_group(running_totals, current_item):
        rows, grads, group_lengths = current_item

        def group_forward(group_rows, params):
            return forward(group_rows, group_lengths, frozen, params)
        output_list, pull = jax.vjp(group_forward, rows, training_step)
        gradient_row_list, grad_train = pull(grads)
        return (jax.tree.map(jnp.add, running_totals, grad_train), (output_list, gradient_row_list))
    zeros = jax.tree.map(jnp.zeros_like, training_step)
    running_totals, (output_list, gradient_row_list) = lax.scan(one_group, zeros, (rows_all, grads_all, lengths_all))
    gradient_layernorm_gain, gradient_layernorm_bias, gradient_projection_bias, gradient_adapter_project_first, gradient_adapter_project_second, gradient_adapter_output_first, gradient_adapter_output_second, gradient_hidden_bias, gradient_adapter_up_first, gradient_adapter_up_second, gradient_adapter_down_first, gradient_adapter_down_second, gradient_branch_bias = running_totals
    return (output_list.reshape(TOKEN_SLOTS, MODEL_WIDTH).astype(jnp.bfloat16), gradient_row_list.reshape(TOKEN_SLOTS, MODEL_WIDTH), gradient_layernorm_gain, gradient_layernorm_bias, gradient_projection_bias, gradient_adapter_project_first, gradient_adapter_project_second, gradient_adapter_output_first, gradient_adapter_output_second, gradient_hidden_bias, gradient_adapter_up_first, gradient_adapter_up_second, gradient_adapter_down_first, gradient_adapter_down_second, gradient_branch_bias)
```

```python
from functools import partial
import math

import jax
import jax.numpy as jnp
from jax import lax
from jax.sharding import PartitionSpec as P

HD = 64
ADAPTER_RANK = 128
ADAPTER_ALPHA = 32
ROW_LEN = 1024
SEQS = 2


NORM_EPSILON = 1e-05
NEG_FILL = -1e30


def matrix_product(left, right):
    return jnp.dot(left, right, preferred_element_type=jnp.float32)


def rotary_tables():
    turned = HD // 4
    half_turn = turned // 2
    freqs = 10000.0 ** (-(jnp.arange(half_turn, dtype=jnp.float32) * 2.0 / turned))
    angles = jnp.arange(ROW_LEN, dtype=jnp.float32)[:, None] * freqs[None, :]
    return (jnp.cos(angles)[:, None, :], jnp.sin(angles)[:, None, :])


def turn(values, cosine, sine):
    half_turn = cosine.shape[-1]
    first = values[..., :half_turn]
    second = values[..., half_turn : 2 * half_turn]
    rest = values[..., 2 * half_turn :]
    return jnp.concatenate(
        [first * cosine - second * sine, second * cosine + first * sine, rest], axis=-1
    )


def layernorm_forward(rows):
    values = rows.astype(jnp.float32)
    centered_rows = values - jnp.mean(values, axis=-1, keepdims=True)
    inverse_scale = lax.rsqrt(
        jnp.mean(centered_rows * centered_rows, axis=-1, keepdims=True) + NORM_EPSILON
    )
    return (centered_rows * inverse_scale, inverse_scale)


def block_scores(queries, keys, offset):
    score_scale = 1.0 / math.sqrt(queries.shape[-1])
    raw = (
        jnp.einsum("qhd,khd->hqk", queries, keys, preferred_element_type=jnp.float32) * score_scale
    )
    query_pos = offset + jnp.arange(queries.shape[0])
    allowed = jnp.arange(keys.shape[0])[None, :] <= query_pos[:, None]
    return (jnp.where(allowed[None], raw, NEG_FILL), allowed, query_pos, score_scale)


def attend_block(queries, keys, values, offset, length):
    scores, allowed, query_pos, score_scale = block_scores(queries, keys, offset)
    peak = jnp.max(scores, axis=-1, keepdims=True)
    powers = jnp.exp(scores - peak)
    running_totals = jnp.sum(powers, axis=-1, keepdims=True)
    weights = (powers / running_totals).astype(jnp.bfloat16)
    attention_context = jnp.einsum(
        "hqk,khd->qhd", weights, values, preferred_element_type=jnp.float32
    )
    valid = (query_pos < length).astype(jnp.float32)
    return (
        (attention_context * valid[:, None, None]).astype(jnp.bfloat16),
        (peak + jnp.log(running_totals))[..., 0],
    )


def attend_block_back(queries, keys, values, gradient_context_rows, log_totals, offset, length):
    scores, allowed, query_pos, score_scale = block_scores(queries, keys, offset)
    weights = jnp.where(allowed[None], jnp.exp(scores - log_totals[..., None]), 0.0)
    valid = (query_pos < length).astype(jnp.bfloat16)
    grad_masked = gradient_context_rows * valid[:, None, None]
    grad_weights = jnp.einsum(
        "qhd,khd->hqk", grad_masked, values, preferred_element_type=jnp.float32
    )
    grad_values = jnp.einsum(
        "hqk,qhd->khd",
        weights.astype(jnp.bfloat16),
        grad_masked,
        preferred_element_type=jnp.float32,
    )
    mean_term = jnp.sum(weights * grad_weights, axis=-1, keepdims=True)
    grad_scores = (weights * (grad_weights - mean_term)).astype(jnp.bfloat16)
    grad_queries = (
        jnp.einsum("hqk,khd->qhd", grad_scores, keys, preferred_element_type=jnp.float32)
        * score_scale
    )
    grad_keys = (
        jnp.einsum("hqk,qhd->khd", grad_scores, queries, preferred_element_type=jnp.float32)
        * score_scale
    )
    return (grad_queries, grad_keys, grad_values)


def attend_row(row):
    queries, keys, values, length = row
    block = queries.shape[0] // 2
    first, first_total = attend_block(queries[:block], keys[:block], values[:block], 0, length)

    def later():
        return attend_block(queries[block:], keys, values, block, length)

    second, second_total = later()
    return (jnp.concatenate([first, second], axis=0), jnp.stack([first_total, second_total]))


def attend_row_back(row):
    queries, keys, values, gradient_context_rows, log_totals, length = row
    block = queries.shape[0] // 2
    first_q, first_k, first_v = attend_block_back(
        queries[:block],
        keys[:block],
        values[:block],
        gradient_context_rows[:block],
        log_totals[0],
        0,
        length,
    )

    def later():
        return attend_block_back(
            queries[block:],
            keys,
            values,
            gradient_context_rows[block:],
            log_totals[1],
            block,
            length,
        )

    second_q, second_k, second_v = later()
    padding = ((0, block), (0, 0), (0, 0))
    grad_queries = jnp.concatenate([first_q, second_q], axis=0)
    grad_keys = second_k + jnp.pad(first_k, padding)
    grad_values = second_v + jnp.pad(first_v, padding)
    return (grad_queries, grad_keys, grad_values)


def shards(
    layer_input_rows,
    cotangent,
    lengths,
    layernorm_gain,
    layernorm_bias,
    frozen_projection_weight,
    projection_bias,
    adapter_project_first,
    adapter_project_second,
    frozen_output_weight,
    adapter_output_first,
    adapter_output_second,
    frozen_up_weight,
    hidden_bias,
    adapter_up_first,
    adapter_up_second,
    frozen_down_weight,
    adapter_down_first,
    adapter_down_second,
    branch_output_bias,
):
    low = jnp.bfloat16
    f32 = jnp.float32
    scale = ADAPTER_ALPHA / ADAPTER_RANK
    n_dp = lax.axis_size("dp")
    n_head = lax.axis_size("head")
    width = layer_input_rows.shape[1]
    head_width = frozen_projection_weight.shape[2]
    heads_local = head_width // HD
    hidden = frozen_up_weight.shape[1]
    depth = frozen_projection_weight.shape[0]
    factor_rows = adapter_project_second.shape[1]
    own_rows = adapter_up_first.shape[0]
    group_rows = SEQS * ROW_LEN
    rank = ADAPTER_RANK

    rows_all = lax.all_gather(layer_input_rows, "head", axis=0, tiled=True)

    main = jnp.concatenate(
        [
            jnp.concatenate(
                [
                    frozen_projection_weight.astype(low).reshape(depth, 3 * head_width),
                    frozen_up_weight.astype(low),
                    frozen_output_weight.astype(low).T,
                    frozen_down_weight.astype(low).T,
                ],
                axis=1,
            ),
            jnp.concatenate(
                [
                    adapter_project_second.astype(low).transpose(1, 0, 2).reshape(factor_rows, 3 * head_width),
                    adapter_up_second.astype(low),
                    adapter_output_first.astype(low).T,
                    adapter_down_first.astype(low).T,
                ],
                axis=1,
            ),
        ],
        axis=0,
    )
    shared = jnp.concatenate(
        [
            adapter_project_first.astype(low).reshape(3 * own_rows, rank),
            adapter_up_first.astype(low),
            adapter_output_second.astype(low).T,
            adapter_down_second.astype(low).T,
        ],
        axis=0,
    )
    small = jnp.stack([layernorm_gain, layernorm_bias, branch_output_bias]).astype(low).reshape(-1)
    biases = jnp.concatenate([projection_bias.astype(low).reshape(-1), hidden_bias.astype(low).reshape(-1)])

    def as_rows(flat):
        count = -(-flat.shape[0] // (16 * rank)) * 16 * rank
        return jnp.pad(flat, (0, count - flat.shape[0])).reshape(-1, rank)

    shared = jnp.concatenate([shared, as_rows(small)], axis=0)
    shared_rows = shared.shape[0]
    shared = lax.all_gather(shared, "head", axis=0, tiled=True)
    shared = jnp.concatenate([shared, as_rows(biases)], axis=0)
    shared = lax.all_gather(shared, "dp", axis=0, tiled=False)
    main = lax.all_gather(main, "dp", axis=0, tiled=False)

    bias_part = shared[:, n_head * shared_rows :].reshape(n_dp, -1)
    shared = shared[:, : n_head * shared_rows].reshape(n_dp * n_head, shared_rows, rank)
    span = projection_bias.shape[2]
    n_proj = 3 * heads_local * span
    proj_bias = bias_part[:, :n_proj].reshape(n_dp, 3, heads_local, span).transpose(1, 2, 0, 3).reshape(3 * head_width).astype(f32)
    n_hid = hidden_bias.shape[0] * span
    hid_bias = bias_part[:, n_proj : n_proj + n_hid].reshape(n_dp, -1, span).transpose(1, 0, 2).reshape(hidden).astype(f32)
    three = 3 * own_rows
    proj_first = shared[:, :three].reshape(n_dp * n_head, 3, own_rows, rank).transpose(1, 0, 2, 3).reshape(3, width, rank)
    up_first = shared[:, three : three + own_rows].reshape(width, rank)
    out_second_t = shared[:, three + own_rows : three + 2 * own_rows].reshape(width, rank)
    down_second_t = shared[:, three + 2 * own_rows : three + 3 * own_rows].reshape(width, rank)
    smalls = shared[:, three + 3 * own_rows :].reshape(n_dp * n_head, -1)[:, : 6 * own_rows]
    smalls = smalls.reshape(n_dp * n_head, 3, 2, own_rows).transpose(1, 2, 0, 3).reshape(3, 2, width).astype(f32)
    gain, shift, out_shift = smalls[0], smalls[1], smalls[2]

    frozen = main[:, :depth].reshape(width, -1)
    factors = main[:, depth:].reshape(rank, -1)
    c1, c2, c3 = 3 * head_width, 3 * head_width + hidden, 4 * head_width + hidden
    w_proj, w_up, w_out_t, w_down_t = frozen[:, :c1], frozen[:, c1:c2], frozen[:, c2:c3], frozen[:, c3:]
    proj_second, up_second = factors[:, :c1], factors[:, c1:c2]
    out_first_t, down_first_t = factors[:, c2:c3], factors[:, c3:]

    def mm(left, right):
        return jnp.dot(left, right, preferred_element_type=f32)

    def mm_t(left, right):
        return lax.dot_general(left, right, (((1,), (1,)), ((), ())), preferred_element_type=f32)

    def tmm(left, right):
        return lax.dot_general(left, right, (((0,), (0,)), ((), ())), preferred_element_type=f32)

    standard, inverse = layernorm_forward(rows_all)
    normed_a = (standard * gain[0] + shift[0]).astype(low)
    normed_m = (standard * gain[1] + shift[1]).astype(low)
    low_qkv = [mm(normed_a, proj_first[c]).astype(low) for c in range(3)]
    cosine, sine = rotary_tables()
    projected = []
    for c in range(3):
        cut = slice(c * head_width, (c + 1) * head_width)
        part = mm(normed_a, w_proj[:, cut]) + proj_bias[cut] + scale * mm(low_qkv[c], proj_second[:, cut])
        part = part.reshape(SEQS, ROW_LEN, heads_local, HD)
        projected.append((turn(part, cosine, sine) if c < 2 else part).astype(low))
    queries, keys, values = projected
    context, log_totals = lax.map(attend_row, (queries, keys, values, lengths))
    context = context.reshape(group_rows, head_width)
    attn_low = mm_t(context, out_first_t).astype(low)
    up_low = mm(normed_m, up_first).astype(low)
    preact = mm(normed_m, w_up) + hid_bias + scale * mm(up_low, up_second)
    units = jax.nn.gelu(preact, approximate=False).astype(low)
    down_low = mm_t(units, down_first_t).astype(low)
    branch = mm_t(context, w_out_t) + mm_t(units, w_down_t)
    branch = branch + scale * (mm_t(attn_low, out_second_t) + mm_t(down_low, down_second_t))
    branch_sum = lax.psum_scatter(branch.astype(low), "head", scatter_dimension=0, tiled=True)
    layer_output = (
        layer_input_rows.astype(f32) + branch_sum.astype(f32) + out_shift[0] + out_shift[1]
    ).astype(low)

    cot = lax.all_gather(cotangent, "head", axis=0, tiled=True)
    g_attn_low = (scale * mm(cot, out_second_t)).astype(low)
    g_down_low = (scale * mm(cot, down_second_t)).astype(low)
    d_out_first_t = tmm(g_attn_low, context)
    d_out_second_t = scale * tmm(cot, attn_low)
    d_down_first_t = tmm(g_down_low, units)
    d_down_second_t = scale * tmm(cot, down_low)
    g_context = (mm(cot, w_out_t) + mm(g_attn_low, out_first_t)).astype(low)
    g_hidden = mm(cot, w_down_t) + mm(g_down_low, down_first_t)
    _, pull = jax.vjp(partial(jax.nn.gelu, approximate=False), preact)
    g_pre = pull(g_hidden)[0].astype(low)
    d_hid_bias = jnp.sum(g_pre, axis=0, dtype=f32)
    d_up_second = scale * tmm(up_low, g_pre)
    g_up_low = (scale * mm_t(g_pre, up_second)).astype(low)
    d_up_first = tmm(normed_m, g_up_low)
    g_normed_m = mm_t(g_pre, w_up) + mm_t(g_up_low, up_first)
    g_rows = g_context.reshape(SEQS, ROW_LEN, heads_local, HD)
    g_q, g_k, g_v = lax.map(attend_row_back, (queries, keys, values, g_rows, log_totals, lengths))
    g_parts = [turn(g_q, cosine, -sine), turn(g_k, cosine, -sine), g_v]
    g_parts = [g.reshape(group_rows, head_width).astype(low) for g in g_parts]
    d_proj_bias = jnp.concatenate([jnp.sum(g, axis=0, dtype=f32) for g in g_parts])
    g_normed_a = 0.0
    d_proj_second, d_proj_first = [], []
    for c in range(3):
        cut = slice(c * head_width, (c + 1) * head_width)
        g = g_parts[c]
        d_proj_second.append(scale * tmm(low_qkv[c], g))
        g_low = (scale * mm_t(g, proj_second[:, cut])).astype(low)
        d_proj_first.append(tmm(normed_a, g_low))
        g_normed_a = g_normed_a + mm_t(g, w_proj[:, cut]) + mm_t(g_low, proj_first[c])
    g_standard = (g_normed_a * gain[0] + g_normed_m * gain[1]).astype(low)
    d_gain = jnp.stack([jnp.sum(g_normed_a * standard, 0), jnp.sum(g_normed_m * standard, 0)])
    d_shift = jnp.stack([jnp.sum(g_normed_a, 0), jnp.sum(g_normed_m, 0)])
    cot_own = cotangent.astype(f32)
    bias_row = jnp.sum(cot_own, axis=0)
    d_branch = jnp.stack([bias_row, bias_row])

    g_own = lax.psum_scatter(g_standard, "head", scatter_dimension=0, tiled=True).astype(f32)
    own_standard, own_inverse = layernorm_forward(layer_input_rows)
    inner = g_own - jnp.mean(g_own, axis=-1, keepdims=True)
    inner = inner - own_standard * jnp.mean(g_own * own_standard, axis=-1, keepdims=True)
    grad_input = cot_own + own_inverse * inner

    per_head = jnp.concatenate(d_proj_second + [d_up_second, d_out_first_t, d_down_first_t], axis=1)
    all_rows = n_dp * n_head
    small = jnp.stack([d_gain, d_shift, d_branch]).reshape(3, 2, all_rows, own_rows).transpose(2, 0, 1, 3)
    small = small.reshape(all_rows, -1)
    small = jnp.pad(small, ((0, 0), (0, 8 * rank - small.shape[1]))).reshape(all_rows, 8, rank)
    shared = jnp.concatenate(
        [
            jnp.stack(d_proj_first).reshape(3, all_rows, own_rows, rank).transpose(1, 0, 2, 3).reshape(all_rows, 3 * own_rows, rank),
            d_up_first.reshape(all_rows, own_rows, rank),
            d_out_second_t.reshape(all_rows, own_rows, rank),
            d_down_second_t.reshape(all_rows, own_rows, rank),
            small,
        ],
        axis=1,
    )
    count = shared.shape[1]
    biases = jnp.concatenate(
        [
            d_proj_bias.reshape(3 * heads_local, n_dp, span).transpose(1, 0, 2).reshape(n_dp, -1),
            d_hid_bias.reshape(-1, n_dp, span).transpose(1, 0, 2).reshape(n_dp, -1),
        ],
        axis=1,
    )
    n_bias = biases.shape[1]
    bias_rows = -(-n_bias // (8 * rank)) * 8
    biases = jnp.pad(biases, ((0, 0), (0, bias_rows * rank - n_bias))).reshape(n_dp, bias_rows, rank)
    shared = jnp.concatenate([shared.reshape(n_dp, n_head * count, rank), biases], axis=1)
    per_head = lax.psum_scatter(per_head, "dp", scatter_dimension=0, tiled=True)
    shared = lax.psum_scatter(shared.reshape(-1, rank), "dp", scatter_dimension=0, tiled=True)
    biases = shared[n_head * count :].reshape(-1)
    shared = lax.psum_scatter(
        shared[: n_head * count], "head", scatter_dimension=0, tiled=True
    )
    small = shared[6 * own_rows :].reshape(-1)[: 6 * own_rows].reshape(3, 2, own_rows)
    return (
        layer_output,
        grad_input,
        small[0],
        small[1],
        biases[:n_proj].reshape(3, heads_local, span),
        shared[: 3 * own_rows].reshape(3, own_rows, rank),
        per_head[:, :c1].reshape(factor_rows, 3, head_width).transpose(1, 0, 2),
        per_head[:, c2:c3].T,
        shared[4 * own_rows : 5 * own_rows].T,
        biases[n_proj : n_proj + n_hid].reshape(-1, span),
        shared[3 * own_rows : 4 * own_rows],
        per_head[:, c1:c2],
        per_head[:, c3:].T,
        shared[5 * own_rows : 6 * own_rows].T,
        small[2],
    )


def solution(mesh):
    in_specs = (
        P(("dp", "head"), None),
        P(("dp", "head"), None),
        P("dp"),
        P(None, ("dp", "head")),
        P(None, ("dp", "head")),
        P("dp", None, "head"),
        P(None, "head", "dp"),
        P(None, ("dp", "head"), None),
        P(None, "dp", "head"),
        P("head", "dp"),
        P("head", "dp"),
        P(None, ("dp", "head")),
        P("dp", "head"),
        P("head", "dp"),
        P(("dp", "head"), None),
        P("dp", "head"),
        P("head", "dp"),
        P("head", "dp"),
        P(None, ("dp", "head")),
        P(None, ("dp", "head")),
    )
    out_specs = (
        P(("dp", "head"), None),
        P(("dp", "head"), None),
        P(None, ("dp", "head")),
        P(None, ("dp", "head")),
        P(None, "head", "dp"),
        P(None, ("dp", "head"), None),
        P(None, "dp", "head"),
        P("head", "dp"),
        P(None, ("dp", "head")),
        P("head", "dp"),
        P(("dp", "head"), None),
        P("dp", "head"),
        P("head", "dp"),
        P(None, ("dp", "head")),
        P(None, ("dp", "head")),
    )
    return jax.shard_map(shards, mesh=mesh, in_specs=in_specs, out_specs=out_specs, check_vma=False)
```
